128 devices in a mesh: grp: 2 (over x_lo), blk: 64 (over y, x_hi, z, core).
Axes of the slice: x: 4 (x_hi: 2, x_lo: 2; x = x_hi * 2 + x_lo), y: 4, z: 4, core: 2. Of those that a mesh axis runs over, the one named last changes fastest.
Arguments:
- zonal_velocity_field: bfloat16 [2048, 64, 128], P('blk'), may hold values from -6 to 6
- meridional_velocity_field: bfloat16 [2048, 64, 128], P('blk'), may hold values from -6 to 6
- barometric_disturbance: bfloat16 [2048, 64, 128], P('blk'), may hold values from -6 to 6
- delayed_thermal_deviation: bfloat16 [2048, 64, 128], P('blk'), may hold values from -6 to 6
- delayed_moisture_deviation: bfloat16 [2048, 64, 128], P('blk'), may hold values from -6 to 6
- flow_category_label: int32 [2048, 64], P('blk'), may hold values from 0 to 63, as said below
- advective_stability_number: float32 [128], replicated, may hold values from 0.25 to 1.3
- initial_dense_matrix: bfloat16 [64, 256, 1024], P('blk'), may hold values from -0.5 to 0.5
- middle_dense_matrix: bfloat16 [64, 1024, 1024], P('blk'), may hold values from -0.25 to 0.25
- closing_dense_matrix: bfloat16 [64, 1024, 1024], P('blk'), may hold values from -0.25 to 0.25
- final_readout_matrix: bfloat16 [64, 1024, 256], P('blk'), may hold values from -0.25 to 0.25
Outputs:
- new_east: bfloat16 [2048, 64, 128], P('blk', 'grp')
- new_north: bfloat16 [2048, 64, 128], P('blk', 'grp')
- new_pressure: bfloat16 [2048, 64, 128], P('blk', 'grp')
- heating: bfloat16 [2048, 64, 128], P('blk', 'grp')
- moistening: bfloat16 [2048, 64, 128], P('blk', 'grp')
The draws below stay inside these ranges and needn't reach their ends.
Inputs may be any that keep to these rules, and one draw needn't show every extreme that they name: Each tile block, rows 32 * b to 32 * b + 31 of flow_category_label, holds exactly 32 columns of every regime.
All inputs are finite; a program needn't handle non-finite values.
Results may differ from the reference program's by a relative error of at most 0.012.
Values may be sent and summed in bfloat16 or wider, within the bound.
A program may use at most 64 MiB of HBM per device.

```python
import math
import jax
import jax.numpy as jnp
from jax import lax

CX = 32
MERIDIAN_COUNT = 64
HEIGHT_COUNT = 128
HID = 1024
SUB = 4
ZONAL_COUNT = 2048
REGIMES = 64


def draw_flow_category_label(key, part):
    blocks = ZONAL_COUNT // CX
    per_block = CX * MERIDIAN_COUNT
    share = per_block // blocks
    block_keys = jax.random.split(jax.random.fold_in(key, 17), blocks)
    shuffled = jax.vmap(lambda block_key: jax.random.permutation(block_key, per_block))(block_keys)
    return (shuffled // share).astype(jnp.int32).reshape(blocks * CX, MERIDIAN_COUNT)


def level_of(rng, extent, cuts, least, high):
    level, own = 1.0, jax.random.fold_in(rng, 6)
    for axis_at, shards_of in cuts:
        steps = jnp.exp(jax.random.uniform(jax.random.fold_in(own, axis_at), (shards_of,), jnp.float32, least / len(cuts), high / len(cuts)))
        level = level * jnp.repeat(steps, extent[axis_at] // shards_of).reshape([-1 if axis == axis_at else 1 for axis in range(len(extent))])
    return level


def gaussian(key, shape, spread, bound, pieces=(), kind=jnp.bfloat16):
    array = jax.random.normal(key, shape, jnp.float32) * spread
    if len(pieces) > 0:
        array = level_of(key, shape, pieces, -0.22, 0.18) * array
    return jnp.clip(array, min=-bound, max=bound).astype(kind)


def setup_inputs(seed: int = 0) -> dict:
    keys = jax.random.split(jax.random.key(seed), 12)
    return {
        "zonal_velocity_field": gaussian(keys[0], (ZONAL_COUNT, MERIDIAN_COUNT, HEIGHT_COUNT), 1.0, 6.0, ((0, 64),)),
        "meridional_velocity_field": gaussian(keys[1], (ZONAL_COUNT, MERIDIAN_COUNT, HEIGHT_COUNT), 1.0, 6.0, ((0, 64),)),
        "barometric_disturbance": gaussian(keys[2], (ZONAL_COUNT, MERIDIAN_COUNT, HEIGHT_COUNT), 1.0, 6.0, ((0, 64),)),
        "delayed_thermal_deviation": gaussian(keys[3], (ZONAL_COUNT, MERIDIAN_COUNT, HEIGHT_COUNT), 1.0, 6.0, ((0, 64),)),
        "delayed_moisture_deviation": gaussian(keys[4], (ZONAL_COUNT, MERIDIAN_COUNT, HEIGHT_COUNT), 1.0, 6.0, ((0, 64),)),
        "flow_category_label": draw_flow_category_label(jax.random.fold_in(keys[11], 71), 0),
        "advective_stability_number": jnp.clip(jnp.exp(jax.random.uniform(keys[6], (HEIGHT_COUNT,), jnp.float32, math.log(0.25), math.log(1.3))), 0.25, 1.3),
        "initial_dense_matrix": gaussian(keys[7], (REGIMES, 2 * HEIGHT_COUNT, HID), HEIGHT_COUNT ** -0.5, 0.5, ((0, 64),)),
        "middle_dense_matrix": gaussian(keys[8], (REGIMES, HID, HID), (HID // 2) ** -0.5, 0.25, ((0, 64),)),
        "closing_dense_matrix": gaussian(keys[9], (REGIMES, HID, HID), (HID // 2) ** -0.5, 0.25, ((0, 64),)),
        "final_readout_matrix": gaussian(keys[10], (REGIMES, HID, 2 * HEIGHT_COUNT), (HID // 2) ** -0.5, 0.25, ((0, 64),)),
    }


def along_cycle(field):
    return (jnp.roll(field, -1, 0) - jnp.roll(field, 1, 0)) * 0.5


def across_belt(field):
    padded = jnp.pad(field, ((0, 0), (1, 1), (0, 0)))
    return (padded[:, 2:] - padded[:, :-2]) * 0.5


def network(inputs):
    columns, first, second, third, last = inputs
    hidden = jax.nn.silu(jnp.dot(columns, first, preferred_element_type=jnp.float32)).astype(jnp.bfloat16)
    hidden = jax.nn.silu(jnp.dot(hidden, second, preferred_element_type=jnp.float32)).astype(jnp.bfloat16)
    hidden = jax.nn.silu(jnp.dot(hidden, third, preferred_element_type=jnp.float32)).astype(jnp.bfloat16)
    return jnp.dot(hidden, last, preferred_element_type=jnp.float32).astype(jnp.bfloat16)


def reference(zonal_velocity_field, meridional_velocity_field, barometric_disturbance, delayed_thermal_deviation, delayed_moisture_deviation, flow_category_label, advective_stability_number, initial_dense_matrix, middle_dense_matrix, closing_dense_matrix, final_readout_matrix):
    courant_rate = advective_stability_number.astype(jnp.float32)
    eastward = zonal_velocity_field.astype(jnp.float32)
    northward = meridional_velocity_field.astype(jnp.float32)
    pressure_state = barometric_disturbance.astype(jnp.float32)
    for substep in range(SUB):
        eastward = eastward - courant_rate * along_cycle(pressure_state)
        northward = northward - courant_rate * across_belt(pressure_state)
        pressure_state = pressure_state - courant_rate * (along_cycle(eastward) + across_belt(northward))
    atmosphere_soundings = jnp.concatenate([delayed_thermal_deviation, delayed_moisture_deviation], axis=-1).reshape(ZONAL_COUNT * MERIDIAN_COUNT, 2 * HEIGHT_COUNT)
    sorting = jnp.argsort(flow_category_label.reshape(-1), stable=True)
    batches = jnp.take(atmosphere_soundings, sorting, axis=0).reshape(REGIMES, (ZONAL_COUNT * MERIDIAN_COUNT) // REGIMES, 2 * HEIGHT_COUNT)
    results = lax.map(network, (batches, initial_dense_matrix, middle_dense_matrix, closing_dense_matrix, final_readout_matrix))
    placed = jnp.zeros_like(atmosphere_soundings).at[sorting].set(results.reshape(ZONAL_COUNT * MERIDIAN_COUNT, 2 * HEIGHT_COUNT))
    tendency = placed.reshape(ZONAL_COUNT, MERIDIAN_COUNT, 2 * HEIGHT_COUNT)
    return (eastward.astype(jnp.bfloat16), northward.astype(jnp.bfloat16), pressure_state.astype(jnp.bfloat16), tendency[:, :, :HEIGHT_COUNT], tendency[:, :, HEIGHT_COUNT:])
```

```python
import functools

import jax
import jax.numpy as jnp
from jax import lax
from jax.experimental import pallas as pl
from jax.experimental.pallas import tpu as pltpu
from jax.sharding import PartitionSpec as P

MESH = pl.DeviceIdType.MESH
SUB = 4
HALO = 2 * SUB
CX, HALF, LEV = 32, 32, 128
COLS = 2 * CX * HALF
WJ = HALF + HALO
ROWS = CX + 2 * HALO
PEERS, PIECE = 64, 16
MINE = PEERS * PIECE
CHUNKS = 4
PER = PEERS // CHUNKS
CROWS = PER * PIECE
BF, F32 = jnp.bfloat16, jnp.float32


def silu(s):
    half = s * 0.5
    return half * jnp.tanh(half) + half


def offset(o):
    dy = (o // 4) % 4
    return dy, (o // 2) % 2, (o // 16 - dy + 4) % 4, o % 2


def peer(o, sign, g, b):
    dy, dx, dz, dc = offset(o)
    y = (b // 16 + sign * dy + 4) % 4
    x = (b // 8 + dx) % 2
    z = ((b // 2) % 4 + sign * dz + 4) % 4
    c = (b + dc) % 2
    return {"grp": (g + dx) % 2, "blk": ((y * 2 + x) * 4 + z) * 2 + c}


def slots_of(lab, ot, cum, rank, g, b):
    labels = lab[...]
    sub = lax.broadcasted_iota(jnp.int32, (64, 128), 0)
    for k in range(16):
        hit = jnp.where(labels[k : k + 1, :] == sub, 1.0, 0.0)
        ot[k * 64 : (k + 1) * 64, :] = hit.astype(BF)
    row = lax.broadcasted_iota(jnp.int32, (128, 256), 0)
    col = lax.broadcasted_iota(jnp.int32, (128, 256), 1)
    tri = jnp.where((row < col) | (col >= 128), 1.0, 0.0).astype(BF)
    cum[...] = jnp.dot(ot[...], tri, preferred_element_type=F32)
    base = jnp.zeros((64, 128), F32)
    for k in range(16):
        hit = ot[k * 64 : (k + 1) * 64, :].astype(F32)
        before = cum[k * 64 : (k + 1) * 64, :128] + base
        rank[k : k + 1, :] = jnp.sum(hit * before, axis=0, keepdims=True)
        base = base + cum[k * 64 : (k + 1) * 64, 128:]
    place = rank[...].astype(jnp.int32)
    dy = ((labels >> 4) - b // 16 + 4) & 3
    dx = ((labels >> 3) + b // 8) & 1
    dz = ((labels >> 1) - (b // 2) % 4 + 4) & 3
    dc = (labels + b) & 1
    o = ((dy + dz) & 3) * 16 + dy * 4 + dx * 2 + dc
    side = ((place >> 4) + g + dx) & 1
    return side * MINE + o * PIECE + (place & (PIECE - 1))


def slope(x):
    edge = lax.broadcasted_iota(jnp.int32, x.shape, 0)
    up = jnp.where(edge == x.shape[0] - 1, 0.0, pltpu.roll(x, x.shape[0] - 1, 0))
    down = jnp.where(edge == 0, 0.0, pltpu.roll(x, 1, 0))
    return up - down


def substep(s, rate, east, north, press):
    lo, hi = 2 * (s + 1), ROWS - 2 * (s + 1)
    half = jnp.broadcast_to(rate[...] * 0.5, (WJ, LEV))
    p_lo, p_next = press[lo], press[lo + 1]
    e_before = east[lo - 1] - half * (p_lo - press[lo - 2])
    e_here = east[lo] - half * (p_next - press[lo - 1])
    east[lo - 1] = e_before
    east[lo] = e_here

    def step(i, carry):
        e_before, e_here, p_here, p_next = carry
        p_after = press[i + 2]
        e_next = east[i + 1] - half * (p_after - p_here)
        east[i + 1] = e_next
        n_here = north[i] - half * slope(p_here)
        north[i] = n_here
        press[i] = p_here - half * ((e_next - e_before) + slope(n_here))
        return e_here, e_next, p_next, p_after

    lax.fori_loop(lo, hi, step, (e_before, e_here, p_lo, p_next))


def main_kernel(
    lab, rate, therm, moist, zonal, merid, baro, w1h, w2h, w3h, w4h,
    back, slots, east_o, north_o, press_o,
    prof, pbuf, ot, cum, rank, send, recv, res, hid_a, hid_b, mine, theirs,
    w1, w2, w3, w4, stage, east, north, press,
    load_sem, weight_sem, out_sem, fs_sem, fr_sem, rs_sem, rr_sem, ps_sem, pr_sem, hs_sem, hr_sem,
):
    g = lax.axis_index("grp")
    b = lax.axis_index("blk")
    partner = {"grp": (g + 1) % 2, "blk": b}
    right = {"grp": g, "blk": (b + 1) % 64}
    left = {"grp": g, "blk": (b + 63) % 64}

    loads = []
    for h in range(2):
        for f, src in enumerate((therm, moist)):
            loads.append(
                pltpu.make_async_copy(
                    src.at[:, pl.ds(h * HALF, HALF), :],
                    prof.at[h, :, :, pl.ds(f * LEV, LEV)],
                    load_sem.at[2 * h + f],
                )
            )
    fields = []
    window = pl.multiple_of(g * (HALF - HALO), 8)
    for f, src in enumerate((zonal, merid, baro)):
        fields.append(
            pltpu.make_async_copy(
                src.at[:, pl.ds(window, WJ), :],
                stage.at[f, pl.ds(HALO, CX)],
                load_sem.at[4 + f],
            )
        )
    weights = [
        pltpu.make_async_copy(src.at[0], dst, weight_sem.at[n])
        for n, (src, dst) in enumerate(((w1h, w1), (w2h, w2), (w3h, w3), (w4h, w4)))
    ]
    for copy in loads + fields + weights:
        copy.start()

    barrier = pltpu.get_barrier_semaphore()

    def greet(o, carry):
        pl.semaphore_signal(barrier, inc=1, device_id=peer(o, 1, g, b), device_id_type=MESH)
        return carry

    lax.fori_loop(1, PEERS, greet, 0)
    for other in (partner, left, right):
        pl.semaphore_signal(barrier, inc=1, device_id=other, device_id_type=MESH)

    slot = slots_of(lab, ot, cum, rank, g, b)
    slots[...] = slot
    for copy in loads:
        copy.wait()

    def gather(m, carry):
        want = lax.broadcasted_iota(jnp.int32, (CROWS, 128), 0) + m * CROWS
        for k in range(16):
            hit = jnp.where(slots[k : k + 1, :] == want, 1.0, 0.0)
            pbuf[:, k * 128 : (k + 1) * 128] = hit.astype(BF)
        rows = jnp.dot(pbuf[...], prof[...].reshape(COLS, 2 * LEV), preferred_element_type=F32)
        send[pl.ds(pl.multiple_of(m * CROWS, CROWS), CROWS), :] = rows.astype(BF)
        return carry

    lax.fori_loop(0, CHUNKS, gather, 0)
    recv[0:PIECE, :] = send[0:PIECE, :]
    pl.semaphore_wait(barrier, PEERS - 1 + 3)

    def piece(o):
        return pl.ds(pl.multiple_of(o * PIECE, PIECE), PIECE)

    def forth(o):
        return pltpu.make_async_remote_copy(
            src_ref=send.at[piece(o)],
            dst_ref=recv.at[piece(o)],
            send_sem=fs_sem.at[o],
            recv_sem=fr_sem.at[o],
            device_id=peer(o, 1, g, b),
            device_id_type=MESH,
        )

    def home(o):
        return pltpu.make_async_remote_copy(
            src_ref=res.at[piece(o)],
            dst_ref=mine.at[piece(o)],
            send_sem=rs_sem.at[o],
            recv_sem=rr_sem.at[o],
            device_id=peer(o, -1, g, b),
            device_id_type=MESH,
        )

    def across(k):
        rows = pl.ds(pl.multiple_of(k * CROWS, CROWS), CROWS)
        return pltpu.make_async_remote_copy(
            src_ref=mine.at[rows],
            dst_ref=theirs.at[rows],
            send_sem=ps_sem.at[k],
            recv_sem=pr_sem.at[k],
            device_id=partner,
            device_id_type=MESH,
        )

    def each(first, last, act):
        def body(o, carry):
            act(o)
            return carry

        lax.fori_loop(first, last, body, 0)

    each(1, PEERS, lambda o: forth(o).start())
    for copy in fields:
        copy.wait()
    halos = [
        pltpu.make_async_remote_copy(
            src_ref=stage.at[:, pl.ds(src, HALO)],
            dst_ref=stage.at[:, pl.ds(dst, HALO)],
            send_sem=hs_sem.at[n],
            recv_sem=hr_sem.at[n],
            device_id=other,
            device_id_type=MESH,
        )
        for n, (src, dst, other) in enumerate(((CX, 0, right), (HALO, HALO + CX, left)))
    ]
    for copy in halos:
        copy.start()
    for copy in weights:
        copy.wait()

    def hand_on(k):
        each(jnp.maximum(k * PER, 1), (k + 1) * PER, lambda o: home(o).wait_recv())
        across(k).start()

    def network(k):
        rows = pl.ds(pl.multiple_of(k * CROWS, CROWS), CROWS)
        x = recv[rows, :]
        for n in range(4):
            cut = slice(n * 256, (n + 1) * 256)
            hid_a[:, cut] = silu(jnp.dot(x, w1[:, cut], preferred_element_type=F32)).astype(BF)
        for n in range(4):
            cut = slice(n * 256, (n + 1) * 256)
            hid_b[:, cut] = silu(jnp.dot(hid_a[...], w2[:, cut], preferred_element_type=F32)).astype(BF)
        for n in range(4):
            cut = slice(n * 256, (n + 1) * 256)
            hid_a[:, cut] = silu(jnp.dot(hid_b[...], w3[:, cut], preferred_element_type=F32)).astype(BF)
        res[rows, :] = jnp.dot(hid_a[...], w4[...], preferred_element_type=F32).astype(BF)

    def turn(k, carry):
        each(jnp.maximum(k * PER, 1), (k + 1) * PER, lambda o: forth(o).wait_recv())
        network(k)
        each(jnp.maximum(k * PER, 1), (k + 1) * PER, lambda o: home(o).start())

        @pl.when(k == 0)
        def _():
            mine[0:PIECE, :] = res[0:PIECE, :]

        @pl.when(k >= 1)
        def _():
            hand_on(k - 1)

        return carry

    lax.fori_loop(0, CHUNKS, turn, 0)

    for copy in halos:
        copy.wait()

    def widen(i, carry):
        east[i] = stage[0, i].astype(F32)
        north[i] = stage[1, i].astype(F32)
        press[i] = stage[2, i].astype(F32)
        return carry

    lax.fori_loop(0, ROWS, widen, 0)
    substep(0, rate, east, north, press)
    hand_on(CHUNKS - 1)
    for s in range(1, SUB):
        substep(s, rate, east, north, press)
    own = pl.ds(pl.multiple_of(g * HALO, 8), HALF)

    def narrow(i, carry):
        east_o[i] = east[i + HALO, own].astype(BF)
        north_o[i] = north[i + HALO, own].astype(BF)
        press_o[i] = press[i + HALO, own].astype(BF)
        return carry

    lax.fori_loop(0, CX, narrow, 0)

    each(0, CHUNKS, lambda k: across(k).wait_send())
    out_mine = pltpu.make_async_copy(mine, back.at[pl.ds(0, MINE)], out_sem.at[0])
    out_mine.start()
    each(0, CHUNKS, lambda k: across(k).wait_recv())
    out_theirs = pltpu.make_async_copy(theirs, back.at[pl.ds(MINE, MINE)], out_sem.at[1])
    out_theirs.start()
    each(1, PEERS, lambda o: forth(o).wait_send())
    each(1, PEERS, lambda o: home(o).wait_send())
    out_mine.wait()
    out_theirs.wait()


def place_kernel(slots, back, east, north, press, east_o, north_o, press_o, heat, moist):
    g = lax.axis_index("grp")
    own = slots[pl.ds(pl.multiple_of(g * 8, 8), 8), :].astype(F32)
    columns = jnp.transpose(own).astype(jnp.int32)
    lane = lax.broadcasted_iota(jnp.int32, (128, 2 * MINE), 1)
    for k in range(4):
        hits = [
            jnp.where(columns[:, 2 * k + q : 2 * k + q + 1] == lane, 1.0, 0.0).astype(BF)
            for q in range(2)
        ]
        rows = jnp.dot(jnp.concatenate(hits, axis=0), back[...], preferred_element_type=F32)
        heat[k * 256 : (k + 1) * 256, :] = rows[:, :LEV].astype(BF)
        moist[k * 256 : (k + 1) * 256, :] = rows[:, LEV:].astype(BF)
    east_o[...] = east[...]
    north_o[...] = north[...]
    press_o[...] = press[...]


def local(zonal, merid, baro, therm, moist, labels, rate, w1, w2, w3, w4):
    lab = labels.reshape(CX, 2, HALF).transpose(1, 0, 2).reshape(16, 128)
    vmem = pl.BlockSpec(memory_space=pltpu.VMEM)
    hbm = pl.BlockSpec(memory_space=pl.ANY)
    field = jax.ShapeDtypeStruct((CX, HALF, LEV), BF)
    dma = pltpu.SemaphoreType.DMA
    hid = w2.shape[-1]
    back, slots, east, north, press = pl.pallas_call(
        main_kernel,
        out_shape=(
            jax.ShapeDtypeStruct((2 * MINE, 2 * LEV), BF),
            jax.ShapeDtypeStruct((16, 128), jnp.int32),
            field, field, field,
        ),
        in_specs=[vmem, vmem] + [hbm] * 9,
        out_specs=(hbm, vmem, vmem, vmem, vmem),
        scratch_shapes=[
            pltpu.VMEM((2, CX, HALF, 2 * LEV), BF),
            pltpu.VMEM((CROWS, COLS), BF),
            pltpu.VMEM((1024, 128), BF),
            pltpu.VMEM((1024, 256), F32),
            pltpu.VMEM((16, 128), F32),
            pltpu.VMEM((MINE, 2 * LEV), BF),
            pltpu.VMEM((MINE, 2 * LEV), BF),
            pltpu.VMEM((MINE, 2 * LEV), BF),
            pltpu.VMEM((CROWS, hid), BF),
            pltpu.VMEM((CROWS, hid), BF),
            pltpu.VMEM((MINE, 2 * LEV), BF),
            pltpu.VMEM((MINE, 2 * LEV), BF),
            pltpu.VMEM(w1.shape[1:], BF),
            pltpu.VMEM(w2.shape[1:], BF),
            pltpu.VMEM(w3.shape[1:], BF),
            pltpu.VMEM(w4.shape[1:], BF),
            pltpu.VMEM((3, ROWS, WJ, LEV), BF),
            pltpu.VMEM((ROWS, WJ, LEV), F32),
            pltpu.VMEM((ROWS, WJ, LEV), F32),
            pltpu.VMEM((ROWS, WJ, LEV), F32),
            dma((7,)), dma((4,)), dma((2,)),
            dma((PEERS,)), dma((PEERS,)), dma((PEERS,)), dma((PEERS,)),
            dma((CHUNKS,)), dma((CHUNKS,)), dma((2,)), dma((2,)),
        ],
        compiler_params=pltpu.CompilerParams(
            collective_id=0, has_side_effects=True, vmem_limit_bytes=40 * 1024 * 1024
        ),
        name="main",
    )(lab, rate.reshape(1, LEV), therm, moist, zonal, merid, baro, w1, w2, w3, w4)
    flat = jax.ShapeDtypeStruct((CX * HALF, LEV), BF)
    east, north, press, heat, moistening = pl.pallas_call(
        place_kernel,
        out_shape=(field, field, field, flat, flat),
        in_specs=[vmem] * 5,
        out_specs=(vmem,) * 5,
        compiler_params=pltpu.CompilerParams(vmem_limit_bytes=32 * 1024 * 1024),
        name="place",
    )(slots, back, east, north, press)
    return east, north, press, heat.reshape(CX, HALF, LEV), moistening.reshape(CX, HALF, LEV)


def solution(mesh):
    whole = P("blk", None, None)
    out = P("blk", "grp", None)
    return jax.shard_map(
        local,
        mesh=mesh,
        in_specs=(whole,) * 5 + (P("blk", None), P()) + (whole,) * 4,
        out_specs=(out,) * 5,
        check_vma=False,
    )
```

```python
import functools

import jax
import jax.numpy as jnp
from jax import lax
from jax.experimental import pallas as pl
from jax.experimental.pallas import tpu as pltpu
from jax.sharding import PartitionSpec as P

MESH = pl.DeviceIdType.MESH
SUB = 4
HALO = 2 * SUB
CX, HALF, LEV = 32, 32, 128
COLS = 2 * CX * HALF
WJ = HALF + HALO
ROWS = CX + 2 * HALO
PEERS, PIECE = 64, 16
MINE = PEERS * PIECE
CHUNKS = 4
PER = PEERS // CHUNKS
CROWS = PER * PIECE
BF, F32 = jnp.bfloat16, jnp.float32


def silu(s):
    half = s * 0.5
    return half * jnp.tanh(half) + half


def span(steps):
    dy, dx, dz, dc = steps
    return min(dy, 4 - dy) + min(dz, 4 - dz) + dx + dc * 0.25


def ordered():
    near = sorted(
        ((dy, dx, dz, dc) for dy in range(4) for dx in range(2) for dz in range(4) for dc in range(2)),
        key=span,
    )
    return near[:PER] + near[PER:][::-1]


ORDER = ordered()


def peers(sign, g, b):
    ys = [(b // 16 + sign * d + 4) % 4 * 16 for d in range(4)]
    xs = [(b // 8 + d) % 2 * 8 for d in range(2)]
    zs = [((b // 2) % 4 + sign * d + 4) % 4 * 2 for d in range(4)]
    cs = [(b + d) % 2 for d in range(2)]
    gs = [g, (g + 1) % 2]
    out = []
    for dy, dx, dz, dc in ORDER:
        out.append({"grp": gs[dx], "blk": ys[dy] + xs[dx] + zs[dz] + cs[dc]})
    return out


def table_of(lab):
    lane = lax.broadcasted_iota(jnp.int32, (8, 128), 1)
    rows = [jnp.zeros((8, 128), jnp.int32) for _ in range(2)]
    for q in range(4):
        part = lab[pl.ds(q, 8, stride=4), :]
        wide = jnp.concatenate([part, part], axis=1)
        for h in range(2):
            moved = pltpu.roll(wide, (q - h) % 4 * HALF, 1) if q != h else wide
            rows[h] = jnp.where(lane // HALF == q, moved, rows[h])
    return jnp.concatenate(rows, axis=0)


def slots_of(lab, ot, cum, rank, g, b):
    labels = table_of(lab)
    sub = lax.broadcasted_iota(jnp.int32, (64, 128), 0)
    for k in range(16):
        hit = jnp.where(labels[k : k + 1, :] == sub, 1.0, 0.0)
        ot[k * 64 : (k + 1) * 64, :] = hit.astype(BF)
    row = lax.broadcasted_iota(jnp.int32, (128, 256), 0)
    col = lax.broadcasted_iota(jnp.int32, (128, 256), 1)
    tri = jnp.where((row < col) | (col >= 128), 1.0, 0.0).astype(BF)
    cum[...] = jnp.dot(ot[...], tri, preferred_element_type=F32)
    base = jnp.zeros((64, 128), F32)
    for k in range(16):
        hit = ot[k * 64 : (k + 1) * 64, :].astype(F32)
        before = cum[k * 64 : (k + 1) * 64, :128] + base
        rank[k : k + 1, :] = jnp.sum(hit * before, axis=0, keepdims=True)
        base = base + cum[k * 64 : (k + 1) * 64, 128:]
    place = rank[...].astype(jnp.int32)
    dy = ((labels >> 4) - b // 16 + 4) & 3
    dx = ((labels >> 3) + b // 8) & 1
    dz = ((labels >> 1) - (b // 2) % 4 + 4) & 3
    dc = (labels + b) & 1
    code = ((dy * 2 + dx) * 4 + dz) * 2 + dc
    o = jnp.zeros_like(code)
    for n, (oy, ox, oz, oc) in enumerate(ORDER):
        o = jnp.where(code == ((oy * 2 + ox) * 4 + oz) * 2 + oc, n, o)
    side = ((place >> 4) + g + dx) & 1
    return side * MINE + o * PIECE + (place & (PIECE - 1))


def slope(x):
    edge = lax.broadcasted_iota(jnp.int32, x.shape, 0)
    up = jnp.where(edge == x.shape[0] - 1, 0.0, pltpu.roll(x, x.shape[0] - 1, 0))
    down = jnp.where(edge == 0, 0.0, pltpu.roll(x, 1, 0))
    return up - down


def substep(s, rate, east, north, press):
    lo, hi = 2 * (s + 1), ROWS - 2 * (s + 1)
    half = jnp.broadcast_to(rate[...] * 0.5, (WJ, LEV))
    p_lo, p_next = press[lo], press[lo + 1]
    e_before = east[lo - 1] - half * (p_lo - press[lo - 2])
    e_here = east[lo] - half * (p_next - press[lo - 1])
    east[lo - 1] = e_before
    east[lo] = e_here

    def step(i, carry):
        e_before, e_here, p_here, p_next = carry
        p_after = press[i + 2]
        e_next = east[i + 1] - half * (p_after - p_here)
        east[i + 1] = e_next
        n_here = north[i] - half * slope(p_here)
        north[i] = n_here
        press[i] = p_here - half * ((e_next - e_before) + slope(n_here))
        return e_here, e_next, p_next, p_after

    lax.fori_loop(lo, hi, step, (e_before, e_here, p_lo, p_next))


def main_kernel(
    lab, rate, therm, moist, zonal, merid, baro, w1h, w2h, w3h, w4h,
    east_o, north_o, press_o, heat_o, moist_o,
    slots, back, goal, prof, pbuf, ot, cum, rank, send, recv, res, hid_a, hid_b,
    w1, w2, w3, w4, stage, east, north, press,
    load_sem, weight_sem, fs_sem, fr_sem, rs_sem, rr_sem, ps_sem, pr_sem, hs_sem, hr_sem,
):
    g = lax.axis_index("grp")
    b = lax.axis_index("blk")
    mine, theirs = back.at[pl.ds(0, MINE)], back.at[pl.ds(MINE, MINE)]
    partner = {"grp": (g + 1) % 2, "blk": b}
    right = {"grp": g, "blk": (b + 1) % 64}
    left = {"grp": g, "blk": (b + 63) % 64}

    ahead, behind = peers(1, g, b), peers(-1, g, b)
    barrier = pltpu.get_barrier_semaphore()

    for o in reversed(range(1, PEERS)):
        pl.semaphore_signal(barrier, inc=1, device_id=ahead[o], device_id_type=MESH)
    for other in (partner, left, right):
        pl.semaphore_signal(barrier, inc=1, device_id=other, device_id_type=MESH)

    loads = []
    for h in range(2):
        for f, src in enumerate((therm, moist)):
            loads.append(
                pltpu.make_async_copy(
                    src.at[:, pl.ds(h * HALF, HALF), :],
                    prof.at[h, :, :, pl.ds(f * LEV, LEV)],
                    load_sem.at[2 * h + f],
                )
            )
    fields = []
    window = pl.multiple_of(g * (HALF - HALO), 8)
    for f, src in enumerate((zonal, merid, baro)):
        fields.append(
            pltpu.make_async_copy(
                src.at[:, pl.ds(window, WJ), :],
                stage.at[f, pl.ds(HALO, CX)],
                load_sem.at[4 + f],
            )
        )
    weights = [
        pltpu.make_async_copy(src.at[0], dst, weight_sem.at[n])
        for n, (src, dst) in enumerate(((w1h, w1), (w2h, w2), (w3h, w3), (w4h, w4)))
    ]
    for copy in loads + fields + weights:
        copy.start()

    slot = slots_of(lab, ot, cum, rank, g, b)
    slots[...] = slot
    for copy in loads:
        copy.wait()

    def gather(m, carry):
        want = lax.broadcasted_iota(jnp.int32, (CROWS, 128), 0) + m * CROWS
        for k in range(16):
            hit = jnp.where(slots[k : k + 1, :] == want, 1.0, 0.0)
            pbuf[:, k * 128 : (k + 1) * 128] = hit.astype(BF)
        rows = jnp.dot(pbuf[...], prof[...].reshape(COLS, 2 * LEV), preferred_element_type=F32)
        send[pl.ds(pl.multiple_of(m * CROWS, CROWS), CROWS), :] = rows.astype(BF)
        return carry

    lax.fori_loop(0, CHUNKS, gather, 0)
    recv[0:PIECE, :] = send[0:PIECE, :]
    pl.semaphore_wait(barrier, PEERS - 1 + 3)

    def piece(o):
        return pl.ds(o * PIECE, PIECE)

    def forth(o):
        return pltpu.make_async_remote_copy(
            src_ref=send.at[piece(o)],
            dst_ref=recv.at[piece(o)],
            send_sem=fs_sem.at[o],
            recv_sem=fr_sem.at[o],
            device_id=ahead[o],
            device_id_type=MESH,
        )

    def home(o):
        return pltpu.make_async_remote_copy(
            src_ref=res.at[piece(o)],
            dst_ref=mine.at[piece(o)],
            send_sem=rs_sem.at[o],
            recv_sem=rr_sem.at[o],
            device_id=behind[o],
            device_id_type=MESH,
        )

    def across(k):
        rows = pl.ds(k * CROWS, CROWS)
        return pltpu.make_async_remote_copy(
            src_ref=mine.at[rows],
            dst_ref=theirs.at[rows],
            send_sem=ps_sem.at[k],
            recv_sem=pr_sem.at[k],
            device_id=partner,
            device_id_type=MESH,
        )

    def each(first, last, act):
        for o in range(first, last):
            act(o)

    each(1, PEERS, lambda o: forth(o).start())
    for copy in fields:
        copy.wait()
    halos = [
        pltpu.make_async_remote_copy(
            src_ref=stage.at[:, pl.ds(src, HALO)],
            dst_ref=stage.at[:, pl.ds(dst, HALO)],
            send_sem=hs_sem.at[n],
            recv_sem=hr_sem.at[n],
            device_id=other,
            device_id_type=MESH,
        )
        for n, (src, dst, other) in enumerate(((CX, 0, right), (HALO, HALO + CX, left)))
    ]
    for copy in halos:
        copy.start()
    places = slots[pl.ds(pl.multiple_of(g * 8, 8), 8), :].astype(F32)
    columns = jnp.transpose(places).astype(jnp.int32)
    lane = lax.broadcasted_iota(jnp.int32, (128, 2 * MINE), 1)
    for k in range(8):
        hit = jnp.where(columns[:, k : k + 1] == lane, 1.0, 0.0)
        goal[k * 128 : (k + 1) * 128, :] = hit.astype(BF)
    for copy in weights:
        copy.wait()

    def hand_on(k):
        each(max(k * PER, 1), (k + 1) * PER, lambda o: home(o).wait_recv())
        across(k).start()

    def network(k):
        rows = pl.ds(k * CROWS, CROWS)
        x = recv[rows, :]
        for n in range(4):
            cut = slice(n * 256, (n + 1) * 256)
            hid_a[:, cut] = silu(jnp.dot(x, w1[:, cut], preferred_element_type=F32)).astype(BF)
        for n in range(4):
            cut = slice(n * 256, (n + 1) * 256)
            hid_b[:, cut] = silu(jnp.dot(hid_a[...], w2[:, cut], preferred_element_type=F32)).astype(BF)
        for n in range(4):
            cut = slice(n * 256, (n + 1) * 256)
            hid_a[:, cut] = silu(jnp.dot(hid_b[...], w3[:, cut], preferred_element_type=F32)).astype(BF)
        res[rows, :] = jnp.dot(hid_a[...], w4[...], preferred_element_type=F32).astype(BF)

    for k in range(CHUNKS):
        each(max(k * PER, 1), (k + 1) * PER, lambda o: forth(o).wait_recv())
        network(k)
        each(max(k * PER, 1), (k + 1) * PER, lambda o: home(o).start())
        if k == 0:
            mine[0:PIECE, :] = res[0:PIECE, :]

    for k in range(CHUNKS):
        hand_on(k)
    for copy in halos:
        copy.wait()

    def widen(i, carry):
        east[i] = stage[0, i].astype(F32)
        north[i] = stage[1, i].astype(F32)
        press[i] = stage[2, i].astype(F32)
        return carry

    lax.fori_loop(0, ROWS, widen, 0)
    for s in range(SUB):
        substep(s, rate, east, north, press)
    own = pl.ds(pl.multiple_of(g * HALO, 8), HALF)

    def narrow(i, carry):
        east_o[i] = east[i + HALO, own].astype(BF)
        north_o[i] = north[i + HALO, own].astype(BF)
        press_o[i] = press[i + HALO, own].astype(BF)
        return carry

    lax.fori_loop(0, CX, narrow, 0)

    each(0, CHUNKS, lambda k: across(k).wait())
    for k in range(4):
        cut = slice(k * 256, (k + 1) * 256)
        rows = jnp.dot(goal[cut, :], back[...], preferred_element_type=F32)
        heat_o[cut, :] = rows[:, :LEV].astype(BF)
        moist_o[cut, :] = rows[:, LEV:].astype(BF)
    each(1, PEERS, lambda o: forth(o).wait_send())
    each(1, PEERS, lambda o: home(o).wait_send())


def store_kernel(*refs):
    sources, targets, sem = refs[:5], refs[5:10], refs[10]
    copies = [
        pltpu.make_async_copy(src, dst, sem.at[n])
        for n, (src, dst) in enumerate(zip(sources, targets))
    ]
    for copy in copies:
        copy.start()
    for copy in copies:
        copy.wait()


def local(zonal, merid, baro, therm, moist, labels, rate, w1, w2, w3, w4):
    vmem = pl.BlockSpec(memory_space=pltpu.VMEM)
    hbm = pl.BlockSpec(memory_space=pltpu.HBM)
    field = jax.ShapeDtypeStruct((CX, HALF, LEV), BF)
    dma = pltpu.SemaphoreType.DMA
    hid = w2.shape[-1]
    flat = jax.ShapeDtypeStruct((CX * HALF, LEV), BF)
    kinds = (field, field, field, flat, flat)
    inputs = [
        pltpu.with_memory_space_constraint(a, pltpu.HBM)
        for a in (labels, rate.reshape(1, LEV), therm, moist, zonal, merid, baro, w1, w2, w3, w4)
    ]
    results = pl.pallas_call(
        main_kernel,
        out_shape=kinds,
        in_specs=[vmem, vmem] + [hbm] * 9,
        out_specs=(vmem,) * 5,
        scratch_shapes=[
            pltpu.VMEM((16, 128), jnp.int32),
            pltpu.VMEM((2 * MINE, 2 * LEV), BF),
            pltpu.VMEM((CX * HALF, 2 * MINE), BF),
            pltpu.VMEM((2, CX, HALF, 2 * LEV), BF),
            pltpu.VMEM((CROWS, COLS), BF),
            pltpu.VMEM((1024, 128), BF),
            pltpu.VMEM((1024, 256), F32),
            pltpu.VMEM((16, 128), F32),
            pltpu.VMEM((MINE, 2 * LEV), BF),
            pltpu.VMEM((MINE, 2 * LEV), BF),
            pltpu.VMEM((MINE, 2 * LEV), BF),
            pltpu.VMEM((CROWS, hid), BF),
            pltpu.VMEM((CROWS, hid), BF),
            pltpu.VMEM(w1.shape[1:], BF),
            pltpu.VMEM(w2.shape[1:], BF),
            pltpu.VMEM(w3.shape[1:], BF),
            pltpu.VMEM(w4.shape[1:], BF),
            pltpu.VMEM((3, ROWS, WJ, LEV), BF),
            pltpu.VMEM((ROWS, WJ, LEV), F32),
            pltpu.VMEM((ROWS, WJ, LEV), F32),
            pltpu.VMEM((ROWS, WJ, LEV), F32),
            dma((7,)), dma((4,)),
            dma((PEERS,)), dma((PEERS,)), dma((PEERS,)), dma((PEERS,)),
            dma((CHUNKS,)), dma((CHUNKS,)), dma((2,)), dma((2,)),
        ],
        compiler_params=pltpu.CompilerParams(
            collective_id=0, has_side_effects=True, vmem_limit_bytes=40 * 1024 * 1024
        ),
        name="main",
    )(*inputs)
    east, north, press, heat, moistening = pl.pallas_call(
        store_kernel,
        out_shape=kinds,
        in_specs=[vmem] * 5,
        out_specs=(hbm,) * 5,
        scratch_shapes=[dma((5,))],
        compiler_params=pltpu.CompilerParams(vmem_limit_bytes=4 * 1024 * 1024),
        name="store",
    )(*results)
    return east, north, press, heat.reshape(CX, HALF, LEV), moistening.reshape(CX, HALF, LEV)


def solution(mesh):
    whole = P("blk", None, None)
    out = P("blk", "grp", None)
    return jax.shard_map(
        local,
        mesh=mesh,
        in_specs=(whole,) * 5 + (P("blk", None), P()) + (whole,) * 4,
        out_specs=(out,) * 5,
        check_vma=False,
    )
```

```python
import functools

import jax
import jax.numpy as jnp
from jax import lax
from jax.experimental import pallas as pl
from jax.experimental.pallas import tpu as pltpu
from jax.sharding import PartitionSpec as P

MESH = pl.DeviceIdType.MESH
SUB = 4
HALO = 2 * SUB
CX, HALF, LEV = 32, 32, 128
COLS = 2 * CX * HALF
WJ = HALF + HALO
ROWS = CX + 2 * HALO
PEERS, PIECE = 64, 16
MINE = PEERS * PIECE
CHUNKS = 4
PER = PEERS // CHUNKS
CROWS = PER * PIECE
HANDS = 8
HPER = PEERS // HANDS
HROWS = HPER * PIECE
HALO_TURN = 3
DYN_AT = 8
DIRECT = 16
FIRST, LAST = DIRECT // HPER, (PEERS - PER) // HPER
BF, F32 = jnp.bfloat16, jnp.float32


def silu(s):
    half = s * 0.5
    return half * jnp.tanh(half) + half


def span(steps):
    dy, dx, dz, dc = steps
    return min(dy, 4 - dy) + min(dz, 4 - dz) + dx + dc * 0.25


ORDER = sorted(
    ((dy, dx, dz, dc) for dy in range(4) for dx in range(2) for dz in range(4) for dc in range(2)),
    key=span,
)


def peers(sign, g, b):
    ys = [(b // 16 + sign * d + 4) % 4 * 16 for d in range(4)]
    xs = [(b // 8 + d) % 2 * 8 for d in range(2)]
    zs = [((b // 2) % 4 + sign * d + 4) % 4 * 2 for d in range(4)]
    cs = [(b + d) % 2 for d in range(2)]
    gs = [g, (g + 1) % 2]
    out = []
    for dy, dx, dz, dc in ORDER:
        out.append({"grp": gs[dx], "blk": ys[dy] + xs[dx] + zs[dz] + cs[dc]})
    return out


def table_of(lab):
    lane = lax.broadcasted_iota(jnp.int32, (8, 128), 1)
    rows = [jnp.zeros((8, 128), jnp.int32) for _ in range(2)]
    for q in range(4):
        part = lab[pl.ds(q, 8, stride=4), :]
        wide = jnp.concatenate([part, part], axis=1)
        for h in range(2):
            moved = pltpu.roll(wide, (q - h) % 4 * HALF, 1) if q != h else wide
            rows[h] = jnp.where(lane // HALF == q, moved, rows[h])
    return jnp.concatenate(rows, axis=0)


def slots_of(lab, ot, cum, rank, g, b):
    labels = table_of(lab)
    sub = lax.broadcasted_iota(jnp.int32, (64, 128), 0)
    for k in range(16):
        hit = jnp.where(labels[k : k + 1, :] == sub, 1.0, 0.0)
        ot[k * 64 : (k + 1) * 64, :] = hit.astype(BF)
    row = lax.broadcasted_iota(jnp.int32, (128, 256), 0)
    col = lax.broadcasted_iota(jnp.int32, (128, 256), 1)
    tri = jnp.where((row < col) | (col >= 128), 1.0, 0.0).astype(BF)
    cum[...] = jnp.dot(ot[...], tri, preferred_element_type=F32)
    base = jnp.zeros((64, 128), F32)
    for k in range(16):
        hit = ot[k * 64 : (k + 1) * 64, :].astype(F32)
        before = cum[k * 64 : (k + 1) * 64, :128] + base
        rank[k : k + 1, :] = jnp.sum(hit * before, axis=0, keepdims=True)
        base = base + cum[k * 64 : (k + 1) * 64, 128:]
    place = rank[...].astype(jnp.int32)
    dy = ((labels >> 4) - b // 16 + 4) & 3
    dx = ((labels >> 3) + b // 8) & 1
    dz = ((labels >> 1) - (b // 2) % 4 + 4) & 3
    dc = (labels + b) & 1
    code = ((dy * 2 + dx) * 4 + dz) * 2 + dc
    o = jnp.zeros_like(code)
    for n, (oy, ox, oz, oc) in enumerate(ORDER):
        o = jnp.where(code == ((oy * 2 + ox) * 4 + oz) * 2 + oc, n, o)
    side = ((place >> 4) + g + dx) & 1
    return side * MINE + o * PIECE + (place & (PIECE - 1))


def slope(x):
    edge = lax.broadcasted_iota(jnp.int32, x.shape, 0)
    up = jnp.where(edge == x.shape[0] - 1, 0.0, pltpu.roll(x, x.shape[0] - 1, 0))
    down = jnp.where(edge == 0, 0.0, pltpu.roll(x, 1, 0))
    return up - down


def substep(s, rate, east, north, press):
    lo, hi = 2 * (s + 1), ROWS - 2 * (s + 1)
    half = jnp.broadcast_to(rate[...] * 0.5, (WJ, LEV))
    p_lo, p_next = press[lo], press[lo + 1]
    e_before = east[lo - 1] - half * (p_lo - press[lo - 2])
    e_here = east[lo] - half * (p_next - press[lo - 1])
    east[lo - 1] = e_before
    east[lo] = e_here

    def step(i, carry):
        e_before, e_here, p_here, p_next = carry
        p_after = press[i + 2]
        e_next = east[i + 1] - half * (p_after - p_here)
        east[i + 1] = e_next
        n_here = north[i] - half * slope(p_here)
        north[i] = n_here
        press[i] = p_here - half * ((e_next - e_before) + slope(n_here))
        return e_here, e_next, p_next, p_after

    lax.fori_loop(lo, hi, step, (e_before, e_here, p_lo, p_next))


def main_kernel(
    lab_h, rate_h, therm, moist, zonal, merid, baro, w1h, w2h, w3h, w4h,
    east_o, north_o, press_o, heat_o, moist_o,
    lab, rate, slots, back, goal, acc, prof, ot, cum, rank, send, recv, res, hid_a, hid_b,
    w1, w2, w3, w4, stage, east, north, press,
    table_sem, load_sem, weight_sem, ds_sem, dr_sem, fs_sem, fr_sem, rs_sem, rr_sem, ps_sem, pr_sem, hs_sem, hr_sem,
):
    g = lax.axis_index("grp")
    b = lax.axis_index("blk")
    mine, theirs = back.at[pl.ds(0, MINE)], back.at[pl.ds(MINE, MINE)]
    partner = {"grp": (g + 1) % 2, "blk": b}
    right = {"grp": g, "blk": (b + 1) % 64}
    left = {"grp": g, "blk": (b + 63) % 64}

    ahead, behind = peers(1, g, b), peers(-1, g, b)
    ahead_too, behind_too = [
        [{"grp": (p["grp"] + 1) % 2, "blk": p["blk"]} for p in near[:DIRECT]] for near in (ahead, behind)
    ]
    barrier = pltpu.get_barrier_semaphore()

    for o in reversed(range(1, PEERS)):
        pl.semaphore_signal(barrier, inc=1, device_id=ahead[o], device_id_type=MESH)
    for other in ahead_too + [left, right]:
        pl.semaphore_signal(barrier, inc=1, device_id=other, device_id_type=MESH)

    tables = [
        pltpu.make_async_copy(src, dst, table_sem.at[n])
        for n, (src, dst) in enumerate(((lab_h, lab), (rate_h, rate)))
    ]
    loads = []
    for h in range(2):
        for f, src in enumerate((therm, moist)):
            loads.append(
                pltpu.make_async_copy(
                    src.at[:, pl.ds(h * HALF, HALF), :],
                    prof.at[h, :, :, pl.ds(f * LEV, LEV)],
                    load_sem.at[2 * h + f],
                )
            )
    fields = []
    window = pl.multiple_of(g * (HALF - HALO), 8)
    for f, src in enumerate((zonal, merid, baro)):
        fields.append(
            pltpu.make_async_copy(
                src.at[:, pl.ds(window, WJ), :],
                stage.at[f, pl.ds(HALO, CX)],
                load_sem.at[4 + f],
            )
        )
    weights = [
        pltpu.make_async_copy(src.at[0], dst, weight_sem.at[n])
        for n, (src, dst) in enumerate(((w1h, w1), (w2h, w2), (w3h, w3), (w4h, w4)))
    ]
    for copy in tables + loads + fields + weights:
        copy.start()

    for copy in tables:
        copy.wait()
    slots[...] = slots_of(lab, ot, cum, rank, g, b)
    for copy in loads:
        copy.wait()

    for m in range(CHUNKS):
        want = lax.broadcasted_iota(jnp.int32, (CROWS, 128), 0) + m * CROWS
        hits = [jnp.where(slots[k : k + 1, :] == want, 1.0, 0.0).astype(BF) for k in range(16)]
        rows = jnp.dot(
            jnp.concatenate(hits, axis=1),
            prof[...].reshape(COLS, 2 * LEV),
            preferred_element_type=F32,
        )
        send[m * CROWS : (m + 1) * CROWS, :] = rows.astype(BF)
    recv[0:PIECE, :] = send[0:PIECE, :]
    pl.semaphore_wait(barrier, PEERS - 1 + DIRECT + 2)

    def piece(o):
        return pl.ds(o * PIECE, PIECE)

    def forth(o):
        return pltpu.make_async_remote_copy(
            src_ref=send.at[piece(o)],
            dst_ref=recv.at[piece(o)],
            send_sem=fs_sem,
            recv_sem=fr_sem.at[o // PER],
            device_id=ahead[o],
            device_id_type=MESH,
        )

    def home(o):
        return pltpu.make_async_remote_copy(
            src_ref=res.at[piece(o)],
            dst_ref=mine.at[piece(o)],
            send_sem=rs_sem,
            recv_sem=rr_sem.at[o // HPER],
            device_id=behind[o],
            device_id_type=MESH,
        )

    def direct(o):
        return pltpu.make_async_remote_copy(
            src_ref=res.at[piece(o)],
            dst_ref=theirs.at[piece(o)],
            send_sem=ds_sem,
            recv_sem=dr_sem,
            device_id=behind_too[o],
            device_id_type=MESH,
        )

    def bulk(ref, first, last, send_sem, recv_sem):
        rows = ref.at[pl.ds(first * PIECE, (last - first) * PIECE)]
        return pltpu.make_async_remote_copy(
            src_ref=rows,
            dst_ref=rows,
            send_sem=send_sem,
            recv_sem=recv_sem,
            device_id=partner,
            device_id_type=MESH,
        )

    def across(k):
        rows = pl.ds(k * HROWS, HROWS)
        return pltpu.make_async_remote_copy(
            src_ref=mine.at[rows],
            dst_ref=theirs.at[rows],
            send_sem=ps_sem,
            recv_sem=pr_sem.at[k // LAST],
            device_id=partner,
            device_id_type=MESH,
        )

    def each(first, last, act):
        for o in range(first, last):
            act(o)

    each(1, PEERS, lambda o: forth(o).start())
    for copy in fields:
        copy.wait()
    halos = [
        pltpu.make_async_remote_copy(
            src_ref=stage.at[:, pl.ds(src, HALO)],
            dst_ref=stage.at[:, pl.ds(dst, HALO)],
            send_sem=hs_sem.at[n],
            recv_sem=hr_sem.at[n],
            device_id=other,
            device_id_type=MESH,
        )
        for n, (src, dst, other) in enumerate(((CX, 0, right), (HALO, HALO + CX, left)))
    ]
    places = slots[pl.ds(pl.multiple_of(g * 8, 8), 8), :].astype(F32)
    columns = jnp.transpose(places).astype(jnp.int32)
    lane = lax.broadcasted_iota(jnp.int32, (128, 2 * MINE), 1)
    for k in range(8):
        hit = jnp.where(columns[:, k : k + 1] == lane, 1.0, 0.0)
        goal[k * 128 : (k + 1) * 128, :] = hit.astype(BF)
    for copy in weights:
        copy.wait()

    def hand_on(k):
        bulk(mine, max(k * HPER, 1), (k + 1) * HPER, rs_sem, rr_sem.at[k]).wait_recv()
        across(k).start()

    def network(k):
        rows = pl.ds(k * CROWS, CROWS)
        x = recv[rows, :]
        for n in range(4):
            cut = slice(n * 256, (n + 1) * 256)
            hid_a[:, cut] = silu(jnp.dot(x, w1[:, cut], preferred_element_type=F32)).astype(BF)
        for n in range(4):
            cut = slice(n * 256, (n + 1) * 256)
            hid_b[:, cut] = silu(jnp.dot(hid_a[...], w2[:, cut], preferred_element_type=F32)).astype(BF)
        for n in range(4):
            cut = slice(n * 256, (n + 1) * 256)
            hid_a[:, cut] = silu(jnp.dot(hid_b[...], w3[:, cut], preferred_element_type=F32)).astype(BF)
        res[rows, :] = jnp.dot(hid_a[...], w4[...], preferred_element_type=F32).astype(BF)

    for k in range(CHUNKS):
        bulk(recv, max(k * PER, 1), (k + 1) * PER, fs_sem, fr_sem.at[k]).wait_recv()
        if k == HALO_TURN:
            for copy in halos:
                copy.start()
        network(k)
        each(max(k * PER, 1), (k + 1) * PER, lambda o: home(o).start())
        each(k * PER, min((k + 1) * PER, DIRECT), lambda o: direct(o).start())
        if k == 0:
            mine[0:PIECE, :] = res[0:PIECE, :]

    def widen(i, carry):
        east[i] = stage[0, i].astype(F32)
        north[i] = stage[1, i].astype(F32)
        press[i] = stage[2, i].astype(F32)
        return carry

    own = pl.ds(pl.multiple_of(g * HALO, 8), HALF)

    def narrow(i, carry):
        east_o[i] = east[i + HALO, own].astype(BF)
        north_o[i] = north[i + HALO, own].astype(BF)
        press_o[i] = press[i + HALO, own].astype(BF)
        return carry

    def dynamics():
        for copy in halos:
            copy.wait()
        lax.fori_loop(0, ROWS, widen, 0)
        for s in range(SUB):
            substep(s, rate, east, north, press)
        lax.fori_loop(0, CX, narrow, 0)

    for k in range(FIRST, HANDS):
        if k == DYN_AT:
            dynamics()
        hand_on(k)
    if DYN_AT == HANDS:
        dynamics()
    for k in range(FIRST):
        bulk(mine, max(k * HPER, 1), (k + 1) * HPER, rs_sem, rr_sem.at[k]).wait_recv()
    bulk(theirs, 0, DIRECT, ds_sem, dr_sem).wait_recv()
    bulk(theirs, DIRECT, LAST * HPER, ps_sem, pr_sem.at[0]).wait_recv()
    early = MINE + LAST * HROWS
    for k in range(4):
        cut = slice(k * 256, (k + 1) * 256)
        acc[cut, :] = jnp.dot(goal[cut, :early], back[:early, :], preferred_element_type=F32)
    bulk(theirs, LAST * HPER, PEERS, ps_sem, pr_sem.at[1]).wait_recv()
    for k in range(4):
        cut = slice(k * 256, (k + 1) * 256)
        rows = acc[cut, :] + jnp.dot(goal[cut, early:], back[early:, :], preferred_element_type=F32)
        heat_o[cut, :] = rows[:, :LEV].astype(BF)
        moist_o[cut, :] = rows[:, LEV:].astype(BF)
    bulk(theirs, DIRECT, PEERS, ps_sem, pr_sem.at[0]).wait_send()
    bulk(theirs, 0, DIRECT, ds_sem, dr_sem).wait_send()
    bulk(send, 1, PEERS, fs_sem, fr_sem.at[0]).wait_send()
    bulk(res, 1, PEERS, rs_sem, rr_sem.at[0]).wait_send()


def store_kernel(*refs):
    sources, targets, sem = refs[:5], refs[5:10], refs[10]
    copies = [
        pltpu.make_async_copy(src, dst, sem.at[n])
        for n, (src, dst) in enumerate(zip(sources, targets))
    ]
    for copy in copies:
        copy.start()
    for copy in copies:
        copy.wait()


def local(zonal, merid, baro, therm, moist, labels, rate, w1, w2, w3, w4):
    vmem = pl.BlockSpec(memory_space=pltpu.VMEM)
    hbm = pl.BlockSpec(memory_space=pltpu.HBM)
    field = jax.ShapeDtypeStruct((CX, HALF, LEV), BF)
    dma = pltpu.SemaphoreType.DMA
    hid = w2.shape[-1]
    flat = jax.ShapeDtypeStruct((CX * HALF, LEV), BF)
    kinds = (field, field, field, flat, flat)
    inputs = [
        pltpu.with_memory_space_constraint(a, pltpu.HBM)
        for a in (labels, rate.reshape(1, LEV), therm, moist, zonal, merid, baro, w1, w2, w3, w4)
    ]
    results = pl.pallas_call(
        main_kernel,
        out_shape=kinds,
        in_specs=[hbm] * 11,
        out_specs=(vmem,) * 5,
        scratch_shapes=[
            pltpu.VMEM((CX, 2 * HALF), jnp.int32),
            pltpu.VMEM((1, LEV), F32),
            pltpu.VMEM((16, 128), jnp.int32),
            pltpu.VMEM((2 * MINE, 2 * LEV), BF),
            pltpu.VMEM((CX * HALF, 2 * MINE), BF),
            pltpu.VMEM((CX * HALF, 2 * LEV), F32),
            pltpu.VMEM((2, CX, HALF, 2 * LEV), BF),
            pltpu.VMEM((1024, 128), BF),
            pltpu.VMEM((1024, 256), F32),
            pltpu.VMEM((16, 128), F32),
            pltpu.VMEM((MINE, 2 * LEV), BF),
            pltpu.VMEM((MINE, 2 * LEV), BF),
            pltpu.VMEM((MINE, 2 * LEV), BF),
            pltpu.VMEM((CROWS, hid), BF),
            pltpu.VMEM((CROWS, hid), BF),
            pltpu.VMEM(w1.shape[1:], BF),
            pltpu.VMEM(w2.shape[1:], BF),
            pltpu.VMEM(w3.shape[1:], BF),
            pltpu.VMEM(w4.shape[1:], BF),
            pltpu.VMEM((3, ROWS, WJ, LEV), BF),
            pltpu.VMEM((ROWS, WJ, LEV), F32),
            pltpu.VMEM((ROWS, WJ, LEV), F32),
            pltpu.VMEM((ROWS, WJ, LEV), F32),
            dma((2,)), dma((7,)), dma((4,)), dma, dma,
            dma, dma((CHUNKS,)), dma, dma((HANDS,)),
            dma, dma((2,)), dma((2,)), dma((2,)),
        ],
        compiler_params=pltpu.CompilerParams(
            collective_id=0, has_side_effects=True, vmem_limit_bytes=40 * 1024 * 1024
        ),
        name="main",
    )(*inputs)
    east, north, press, heat, moistening = pl.pallas_call(
        store_kernel,
        out_shape=kinds,
        in_specs=[vmem] * 5,
        out_specs=(hbm,) * 5,
        scratch_shapes=[dma((5,))],
        compiler_params=pltpu.CompilerParams(vmem_limit_bytes=4 * 1024 * 1024),
        name="store",
    )(*results)
    return east, north, press, heat.reshape(CX, HALF, LEV), moistening.reshape(CX, HALF, LEV)


def solution(mesh):
    whole = P("blk", None, None)
    out = P("blk", "grp", None)
    return jax.shard_map(
        local,
        mesh=mesh,
        in_specs=(whole,) * 5 + (P("blk", None), P()) + (whole,) * 4,
        out_specs=(out,) * 5,
        check_vma=False,
    )
```

```python
import functools

import jax
import jax.numpy as jnp
from jax import lax
from jax.experimental import pallas as pl
from jax.experimental.pallas import tpu as pltpu
from jax.sharding import PartitionSpec as P

MESH = pl.DeviceIdType.MESH
SUB = 4
HALO = 2 * SUB
CX, HALF, LEV = 32, 32, 128
COLS = 2 * CX * HALF
WJ = HALF + HALO
ROWS = CX + 2 * HALO
PEERS, PIECE = 64, 16
MINE = PEERS * PIECE
CHUNKS = 4
PER = PEERS // CHUNKS
CROWS = PER * PIECE
HANDS = 8
HPER = PEERS // HANDS
HROWS = HPER * PIECE
DIRECT = 16
FIRST, LAST = DIRECT // HPER, (PEERS - PER) // HPER
BF, F32 = jnp.bfloat16, jnp.float32


def silu(s):
    half = s * 0.5
    return half * jnp.tanh(half) + half


def span(steps):
    dy, dx, dz, dc = steps
    return min(dy, 4 - dy) + min(dz, 4 - dz) + dx + dc * 0.25


ORDER = sorted(
    ((dy, dx, dz, dc) for dy in range(4) for dx in range(2) for dz in range(4) for dc in range(2)),
    key=span,
)


def peers(sign, g, b):
    ys = [(b // 16 + sign * d + 4) % 4 * 16 for d in range(4)]
    xs = [(b // 8 + d) % 2 * 8 for d in range(2)]
    zs = [((b // 2) % 4 + sign * d + 4) % 4 * 2 for d in range(4)]
    cs = [(b + d) % 2 for d in range(2)]
    gs = [g, (g + 1) % 2]
    out = []
    for dy, dx, dz, dc in ORDER:
        out.append({"grp": gs[dx], "blk": ys[dy] + xs[dx] + zs[dz] + cs[dc]})
    return out


def table_of(lab):
    lane = lax.broadcasted_iota(jnp.int32, (8, 128), 1)
    rows = [jnp.zeros((8, 128), jnp.int32) for _ in range(2)]
    for q in range(4):
        part = lab[pl.ds(q, 8, stride=4), :]
        wide = jnp.concatenate([part, part], axis=1)
        for h in range(2):
            moved = pltpu.roll(wide, (q - h) % 4 * HALF, 1) if q != h else wide
            rows[h] = jnp.where(lane // HALF == q, moved, rows[h])
    return jnp.concatenate(rows, axis=0)


def slots_of(lab, ot, cum, rank, g, b):
    labels = table_of(lab)
    sub = lax.broadcasted_iota(jnp.int32, (64, 128), 0)
    for k in range(16):
        hit = jnp.where(labels[k : k + 1, :] == sub, 1.0, 0.0)
        ot[k * 64 : (k + 1) * 64, :] = hit.astype(BF)
    row = lax.broadcasted_iota(jnp.int32, (128, 256), 0)
    col = lax.broadcasted_iota(jnp.int32, (128, 256), 1)
    tri = jnp.where((row < col) | (col >= 128), 1.0, 0.0).astype(BF)
    cum[...] = jnp.dot(ot[...], tri, preferred_element_type=F32)
    base = jnp.zeros((64, 128), F32)
    for k in range(16):
        hit = ot[k * 64 : (k + 1) * 64, :].astype(F32)
        before = cum[k * 64 : (k + 1) * 64, :128] + base
        rank[k : k + 1, :] = jnp.sum(hit * before, axis=0, keepdims=True)
        base = base + cum[k * 64 : (k + 1) * 64, 128:]
    place = rank[...].astype(jnp.int32)
    dy = ((labels >> 4) - b // 16 + 4) & 3
    dx = ((labels >> 3) + b // 8) & 1
    dz = ((labels >> 1) - (b // 2) % 4 + 4) & 3
    dc = (labels + b) & 1
    code = ((dy * 2 + dx) * 4 + dz) * 2 + dc
    o = jnp.zeros_like(code)
    for n, (oy, ox, oz, oc) in enumerate(ORDER):
        o = jnp.where(code == ((oy * 2 + ox) * 4 + oz) * 2 + oc, n, o)
    side = ((place >> 4) + g + dx) & 1
    return side * MINE + o * PIECE + (place & (PIECE - 1))


def slope(x):
    edge = lax.broadcasted_iota(jnp.int32, x.shape, 0)
    up = jnp.where(edge == x.shape[0] - 1, 0.0, pltpu.roll(x, x.shape[0] - 1, 0))
    down = jnp.where(edge == 0, 0.0, pltpu.roll(x, 1, 0))
    return up - down


def advance(half, east, north, press, winds, cells):
    def wind(i, carry):
        east[i] = east[i] - half * (press[i + 1] - press[i - 1])
        return carry

    def cell(i, carry):
        here = press[i]
        wind_north = north[i] - half * slope(here)
        north[i] = wind_north
        press[i] = here - half * ((east[i + 1] - east[i - 1]) + slope(wind_north))
        return carry

    lax.fori_loop(*winds, wind, 0, unroll=2)
    lax.fori_loop(*cells, cell, 0, unroll=2)


def main_kernel(
    lab_h, rate_h, therm, moist, zonal, merid, baro, w1h, w2h, w3h, w4h,
    east_o, north_o, press_o, heat_o, moist_o,
    lab, rate, slots, back, goal, acc, prof, ot, cum, rank, send, recv, res, hid_a, hid_b,
    w1, w2, w3, w4, stage, east, north, press,
    table_sem, load_sem, weight_sem, ds_sem, dr_sem, fs_sem, fr_sem, rs_sem, rr_sem, ps_sem, pr_sem, hs_sem, hr_sem,
):
    g = lax.axis_index("grp")
    b = lax.axis_index("blk")
    mine, theirs = back.at[pl.ds(0, MINE)], back.at[pl.ds(MINE, MINE)]
    partner = {"grp": (g + 1) % 2, "blk": b}
    right = {"grp": g, "blk": (b + 1) % 64}
    left = {"grp": g, "blk": (b + 63) % 64}

    ahead, behind = peers(1, g, b), peers(-1, g, b)
    ahead_too, behind_too = [
        [{"grp": (p["grp"] + 1) % 2, "blk": p["blk"]} for p in near[:DIRECT]] for near in (ahead, behind)
    ]
    tables = [
        pltpu.make_async_copy(src, dst, table_sem.at[n])
        for n, (src, dst) in enumerate(((lab_h, lab), (rate_h, rate)))
    ]
    loads = []
    for h in range(2):
        for f, src in enumerate((therm, moist)):
            loads.append(
                pltpu.make_async_copy(
                    src.at[:, pl.ds(h * HALF, HALF), :],
                    prof.at[h, :, :, pl.ds(f * LEV, LEV)],
                    load_sem.at[2 * h + f],
                )
            )
    for copy in tables + loads:
        copy.start()

    barrier = pltpu.get_barrier_semaphore()

    for o in reversed(range(1, PEERS)):
        pl.semaphore_signal(barrier, inc=1, device_id=ahead[o], device_id_type=MESH)
    for other in ahead_too + [left, right]:
        pl.semaphore_signal(barrier, inc=1, device_id=other, device_id_type=MESH)

    fields = []
    window = pl.multiple_of(g * (HALF - HALO), 8)
    for f, src in enumerate((zonal, merid, baro)):
        fields.append(
            pltpu.make_async_copy(
                src.at[:, pl.ds(window, WJ), :],
                stage.at[f, pl.ds(HALO, CX)],
                load_sem.at[4 + f],
            )
        )
    weights = [
        pltpu.make_async_copy(src.at[0], dst, weight_sem.at[n])
        for n, (src, dst) in enumerate(((w1h, w1), (w2h, w2), (w3h, w3), (w4h, w4)))
    ]
    for copy in fields + weights:
        copy.start()

    for copy in tables:
        copy.wait()
    slots[...] = slots_of(lab, ot, cum, rank, g, b)
    for copy in loads:
        copy.wait()

    for m in range(CHUNKS):
        want = lax.broadcasted_iota(jnp.int32, (CROWS, 128), 0) + m * CROWS
        hits = [jnp.where(slots[k : k + 1, :] == want, 1.0, 0.0).astype(BF) for k in range(16)]
        rows = jnp.dot(
            jnp.concatenate(hits, axis=1),
            prof[...].reshape(COLS, 2 * LEV),
            preferred_element_type=F32,
        )
        send[m * CROWS : (m + 1) * CROWS, :] = rows.astype(BF)
    recv[0:PIECE, :] = send[0:PIECE, :]
    pl.semaphore_wait(barrier, PEERS - 1 + DIRECT + 2)

    def piece(o):
        return pl.ds(o * PIECE, PIECE)

    def forth(o):
        return pltpu.make_async_remote_copy(
            src_ref=send.at[piece(o)],
            dst_ref=recv.at[piece(o)],
            send_sem=fs_sem,
            recv_sem=fr_sem.at[o // PER],
            device_id=ahead[o],
            device_id_type=MESH,
        )

    def home(o):
        return pltpu.make_async_remote_copy(
            src_ref=res.at[piece(o)],
            dst_ref=mine.at[piece(o)],
            send_sem=rs_sem,
            recv_sem=rr_sem.at[o // HPER],
            device_id=behind[o],
            device_id_type=MESH,
        )

    def direct(o):
        return pltpu.make_async_remote_copy(
            src_ref=res.at[piece(o)],
            dst_ref=theirs.at[piece(o)],
            send_sem=ds_sem,
            recv_sem=dr_sem,
            device_id=behind_too[o],
            device_id_type=MESH,
        )

    def bulk(ref, first, last, send_sem, recv_sem):
        rows = ref.at[pl.ds(first * PIECE, (last - first) * PIECE)]
        return pltpu.make_async_remote_copy(
            src_ref=rows,
            dst_ref=rows,
            send_sem=send_sem,
            recv_sem=recv_sem,
            device_id=partner,
            device_id_type=MESH,
        )

    def across(k):
        rows = pl.ds(k * HROWS, HROWS)
        return pltpu.make_async_remote_copy(
            src_ref=mine.at[rows],
            dst_ref=theirs.at[rows],
            send_sem=ps_sem,
            recv_sem=pr_sem.at[k // LAST],
            device_id=partner,
            device_id_type=MESH,
        )

    def each(first, last, act):
        for o in range(first, last):
            act(o)

    each(1, PEERS, lambda o: forth(o).start())
    halos = [
        pltpu.make_async_remote_copy(
            src_ref=stage.at[:, pl.ds(src, HALO)],
            dst_ref=stage.at[:, pl.ds(dst, HALO)],
            send_sem=hs_sem.at[n],
            recv_sem=hr_sem.at[n],
            device_id=other,
            device_id_type=MESH,
        )
        for n, (src, dst, other) in enumerate(((CX, 0, right), (HALO, HALO + CX, left)))
    ]
    places = slots[pl.ds(pl.multiple_of(g * 8, 8), 8), :].astype(F32)
    columns = jnp.transpose(places).astype(jnp.int32)
    lane = lax.broadcasted_iota(jnp.int32, (128, 2 * MINE), 1)
    for k in range(8):
        hit = jnp.where(columns[:, k : k + 1] == lane, 1.0, 0.0)
        goal[k * 128 : (k + 1) * 128, :] = hit.astype(BF)
    for copy in fields:
        copy.wait()

    def widen(i, carry):
        east[i] = stage[0, i].astype(F32)
        north[i] = stage[1, i].astype(F32)
        press[i] = stage[2, i].astype(F32)
        return carry

    half = jnp.broadcast_to(rate[...] * 0.5, (WJ, LEV))
    lax.fori_loop(HALO, HALO + CX, widen, 0)
    for s in range(2, 2 * SUB + 2, 2):
        advance(half, east, north, press, (s + 7, ROWS - 7 - s), (s + 8, ROWS - 8 - s))
    for copy in weights:
        copy.wait()

    def hand_on(k):
        bulk(mine, max(k * HPER, 1), (k + 1) * HPER, rs_sem, rr_sem.at[k]).wait_recv()
        across(k).start()

    def network(k):
        rows = pl.ds(k * CROWS, CROWS)
        x = recv[rows, :]
        for n in range(4):
            cut = slice(n * 256, (n + 1) * 256)
            hid_a[:, cut] = silu(jnp.dot(x, w1[:, cut], preferred_element_type=F32)).astype(BF)
        for n in range(4):
            cut = slice(n * 256, (n + 1) * 256)
            hid_b[:, cut] = silu(jnp.dot(hid_a[...], w2[:, cut], preferred_element_type=F32)).astype(BF)
        for n in range(4):
            cut = slice(n * 256, (n + 1) * 256)
            hid_a[:, cut] = silu(jnp.dot(hid_b[...], w3[:, cut], preferred_element_type=F32)).astype(BF)
        res[rows, :] = jnp.dot(hid_a[...], w4[...], preferred_element_type=F32).astype(BF)

    for k in range(CHUNKS):
        bulk(recv, max(k * PER, 1), (k + 1) * PER, fs_sem, fr_sem.at[k]).wait_recv()
        network(k)
        each(max(k * PER, 1), (k + 1) * PER, lambda o: home(o).start())
        each(k * PER, min((k + 1) * PER, DIRECT), lambda o: direct(o).start())
        if k == 0:
            mine[0:PIECE, :] = res[0:PIECE, :]

    own = pl.ds(pl.multiple_of(g * HALO, 8), HALF)

    def narrow(i, carry):
        east_o[i] = east[i + HALO, own].astype(BF)
        north_o[i] = north[i + HALO, own].astype(BF)
        press_o[i] = press[i + HALO, own].astype(BF)
        return carry

    for copy in halos:
        copy.start()
    for k in range(FIRST, HANDS):
        hand_on(k)
    for copy in halos:
        copy.wait()
    lax.fori_loop(0, HALO, widen, 0)
    lax.fori_loop(HALO + CX, ROWS, widen, 0)
    for s in range(2, 2 * SUB + 2, 2):
        advance(half, east, north, press, (s - 1, s + 7), (s, s + 8))
        advance(half, east, north, press, (ROWS - 7 - s, ROWS + 1 - s), (ROWS - 8 - s, ROWS - s))
    lax.fori_loop(0, CX, narrow, 0)
    for k in range(FIRST):
        bulk(mine, max(k * HPER, 1), (k + 1) * HPER, rs_sem, rr_sem.at[k]).wait_recv()
    bulk(theirs, 0, DIRECT, ds_sem, dr_sem).wait_recv()
    bulk(theirs, DIRECT, LAST * HPER, ps_sem, pr_sem.at[0]).wait_recv()
    early = MINE + LAST * HROWS
    for k in range(4):
        cut = slice(k * 256, (k + 1) * 256)
        acc[cut, :] = jnp.dot(goal[cut, :early], back[:early, :], preferred_element_type=F32)
    bulk(theirs, LAST * HPER, PEERS, ps_sem, pr_sem.at[1]).wait_recv()
    for k in range(4):
        cut = slice(k * 256, (k + 1) * 256)
        rows = acc[cut, :] + jnp.dot(goal[cut, early:], back[early:, :], preferred_element_type=F32)
        heat_o[cut, :] = rows[:, :LEV].astype(BF)
        moist_o[cut, :] = rows[:, LEV:].astype(BF)
    bulk(theirs, DIRECT, PEERS, ps_sem, pr_sem.at[0]).wait_send()
    bulk(theirs, 0, DIRECT, ds_sem, dr_sem).wait_send()
    bulk(send, 1, PEERS, fs_sem, fr_sem.at[0]).wait_send()
    bulk(res, 1, PEERS, rs_sem, rr_sem.at[0]).wait_send()


def store_kernel(*refs):
    sources, targets, sem = refs[:5], refs[5:10], refs[10]
    copies = [
        pltpu.make_async_copy(src, dst, sem.at[n])
        for n, (src, dst) in enumerate(zip(sources, targets))
    ]
    for copy in copies:
        copy.start()
    for copy in copies:
        copy.wait()


def local(zonal, merid, baro, therm, moist, labels, rate, w1, w2, w3, w4):
    vmem = pl.BlockSpec(memory_space=pltpu.VMEM)
    hbm = pl.BlockSpec(memory_space=pltpu.HBM)
    field = jax.ShapeDtypeStruct((CX, HALF, LEV), BF)
    dma = pltpu.SemaphoreType.DMA
    hid = w2.shape[-1]
    flat = jax.ShapeDtypeStruct((CX * HALF, LEV), BF)
    kinds = (field, field, field, flat, flat)
    inputs = [
        pltpu.with_memory_space_constraint(a, pltpu.HBM)
        for a in (labels, rate.reshape(1, LEV), therm, moist, zonal, merid, baro, w1, w2, w3, w4)
    ]
    results = pl.pallas_call(
        main_kernel,
        out_shape=kinds,
        in_specs=[hbm] * 11,
        out_specs=(vmem,) * 5,
        scratch_shapes=[
            pltpu.VMEM((CX, 2 * HALF), jnp.int32),
            pltpu.VMEM((1, LEV), F32),
            pltpu.VMEM((16, 128), jnp.int32),
            pltpu.VMEM((2 * MINE, 2 * LEV), BF),
            pltpu.VMEM((CX * HALF, 2 * MINE), BF),
            pltpu.VMEM((CX * HALF, 2 * LEV), F32),
            pltpu.VMEM((2, CX, HALF, 2 * LEV), BF),
            pltpu.VMEM((1024, 128), BF),
            pltpu.VMEM((1024, 256), F32),
            pltpu.VMEM((16, 128), F32),
            pltpu.VMEM((MINE, 2 * LEV), BF),
            pltpu.VMEM((MINE, 2 * LEV), BF),
            pltpu.VMEM((MINE, 2 * LEV), BF),
            pltpu.VMEM((CROWS, hid), BF),
            pltpu.VMEM((CROWS, hid), BF),
            pltpu.VMEM(w1.shape[1:], BF),
            pltpu.VMEM(w2.shape[1:], BF),
            pltpu.VMEM(w3.shape[1:], BF),
            pltpu.VMEM(w4.shape[1:], BF),
            pltpu.VMEM((3, ROWS, WJ, LEV), BF),
            pltpu.VMEM((ROWS, WJ, LEV), F32),
            pltpu.VMEM((ROWS, WJ, LEV), F32),
            pltpu.VMEM((ROWS, WJ, LEV), F32),
            dma((2,)), dma((7,)), dma((4,)), dma, dma,
            dma, dma((CHUNKS,)), dma, dma((HANDS,)),
            dma, dma((2,)), dma((2,)), dma((2,)),
        ],
        compiler_params=pltpu.CompilerParams(
            collective_id=0, has_side_effects=True, vmem_limit_bytes=40 * 1024 * 1024
        ),
        name="main",
    )(*inputs)
    east, north, press, heat, moistening = pl.pallas_call(
        store_kernel,
        out_shape=kinds,
        in_specs=[vmem] * 5,
        out_specs=(hbm,) * 5,
        scratch_shapes=[dma((5,))],
        compiler_params=pltpu.CompilerParams(vmem_limit_bytes=4 * 1024 * 1024),
        name="store",
    )(*results)
    return east, north, press, heat.reshape(CX, HALF, LEV), moistening.reshape(CX, HALF, LEV)


def solution(mesh):
    whole = P("blk", None, None)
    out = P("blk", "grp", None)
    return jax.shard_map(
        local,
        mesh=mesh,
        in_specs=(whole,) * 5 + (P("blk", None), P()) + (whole,) * 4,
        out_specs=(out,) * 5,
        check_vma=False,
    )
```

```python
import functools

import jax
import jax.numpy as jnp
from jax import lax
from jax.experimental import pallas as pl
from jax.experimental.pallas import tpu as pltpu
from jax.sharding import PartitionSpec as P

MESH = pl.DeviceIdType.MESH
SUB = 4
HALO = 2 * SUB
CX, HALF, LEV = 32, 32, 128
COLS = 2 * CX * HALF
WJ = HALF + HALO
ROWS = CX + 2 * HALO
PEERS, PIECE = 64, 16
MINE = PEERS * PIECE
CHUNKS = 4
PER = PEERS // CHUNKS
CROWS = PER * PIECE
HANDS = 8
HPER = PEERS // HANDS
HROWS = HPER * PIECE
DIRECT = 16
FIRST, LAST = DIRECT // HPER, (PEERS - PER) // HPER
BF, F32 = jnp.bfloat16, jnp.float32


def silu(s):
    half = s * 0.5
    return half * jnp.tanh(half) + half


def span(steps):
    dy, dx, dz, dc = steps
    return min(dy, 4 - dy) + min(dz, 4 - dz) + dx + dc * 0.25


ORDER = sorted(
    ((dy, dx, dz, dc) for dy in range(4) for dx in range(2) for dz in range(4) for dc in range(2)),
    key=span,
)


def peers(sign, g, b):
    ys = [(b // 16 + sign * d + 4) % 4 * 16 for d in range(4)]
    xs = [(b // 8 + d) % 2 * 8 for d in range(2)]
    zs = [((b // 2) % 4 + sign * d + 4) % 4 * 2 for d in range(4)]
    cs = [(b + d) % 2 for d in range(2)]
    gs = [g, (g + 1) % 2]
    out = []
    for dy, dx, dz, dc in ORDER:
        out.append({"grp": gs[dx], "blk": ys[dy] + xs[dx] + zs[dz] + cs[dc]})
    return out


def table_of(lab):
    lane = lax.broadcasted_iota(jnp.int32, (8, 128), 1)
    rows = [jnp.zeros((8, 128), jnp.int32) for _ in range(2)]
    for q in range(4):
        part = lab[pl.ds(q, 8, stride=4), :]
        wide = jnp.concatenate([part, part], axis=1)
        for h in range(2):
            moved = pltpu.roll(wide, (q - h) % 4 * HALF, 1) if q != h else wide
            rows[h] = jnp.where(lane // HALF == q, moved, rows[h])
    return jnp.concatenate(rows, axis=0)


def slots_of(lab, ot, cum, rank, g, b):
    labels = table_of(lab)
    sub = lax.broadcasted_iota(jnp.int32, (64, 128), 0)
    for k in range(16):
        hit = jnp.where(labels[k : k + 1, :] == sub, 1.0, 0.0)
        ot[k * 64 : (k + 1) * 64, :] = hit.astype(BF)
    row = lax.broadcasted_iota(jnp.int32, (128, 256), 0)
    col = lax.broadcasted_iota(jnp.int32, (128, 256), 1)
    tri = jnp.where((row < col) | (col >= 128), 1.0, 0.0).astype(BF)
    cum[...] = jnp.dot(ot[...], tri, preferred_element_type=F32)
    base = jnp.zeros((64, 128), F32)
    for k in range(16):
        hit = ot[k * 64 : (k + 1) * 64, :].astype(F32)
        before = cum[k * 64 : (k + 1) * 64, :128] + base
        rank[k : k + 1, :] = jnp.sum(hit * before, axis=0, keepdims=True)
        base = base + cum[k * 64 : (k + 1) * 64, 128:]
    place = rank[...].astype(jnp.int32)
    dy = ((labels >> 4) - b // 16 + 4) & 3
    dx = ((labels >> 3) + b // 8) & 1
    dz = ((labels >> 1) - (b // 2) % 4 + 4) & 3
    dc = (labels + b) & 1
    code = ((dy * 2 + dx) * 4 + dz) * 2 + dc
    o = jnp.zeros_like(code)
    for n, (oy, ox, oz, oc) in enumerate(ORDER):
        o = jnp.where(code == ((oy * 2 + ox) * 4 + oz) * 2 + oc, n, o)
    side = ((place >> 4) + g + dx) & 1
    return side * MINE + o * PIECE + (place & (PIECE - 1))


def slope(x):
    edge = lax.broadcasted_iota(jnp.int32, x.shape, 0)
    up = jnp.where(edge == x.shape[0] - 1, 0.0, pltpu.roll(x, x.shape[0] - 1, 0))
    down = jnp.where(edge == 0, 0.0, pltpu.roll(x, 1, 0))
    return up - down


def advance(half, east, north, press, winds, cells):
    def wind(i, carry):
        east[i] = east[i] - half * (press[i + 1] - press[i - 1])
        return carry

    def cell(i, carry):
        here = press[i]
        wind_north = north[i] - half * slope(here)
        north[i] = wind_north
        press[i] = here - half * ((east[i + 1] - east[i - 1]) + slope(wind_north))
        return carry

    lax.fori_loop(*winds, wind, 0, unroll=2)
    lax.fori_loop(*cells, cell, 0, unroll=2)


def main_kernel(
    lab_h, rate_h, therm, moist, zonal, merid, baro, w1h, w2h, w3h, w4h,
    east_o, north_o, press_o, heat_o, moist_o,
    lab, rate, slots, back, goal, acc, prof, ot, cum, rank, send, recv, res, hid_a, hid_b,
    w1, w2, w3, w4, stage, east, north, press,
    table_sem, load_sem, weight_sem, ds_sem, dr_sem, fs_sem, fr_sem, rs_sem, rr_sem, ps_sem, pr_sem, hs_sem, hr_sem,
):
    g = lax.axis_index("grp")
    b = lax.axis_index("blk")
    mine, theirs = back.at[pl.ds(0, MINE)], back.at[pl.ds(MINE, MINE)]
    partner = {"grp": (g + 1) % 2, "blk": b}
    right = {"grp": g, "blk": (b + 1) % 64}
    left = {"grp": g, "blk": (b + 63) % 64}

    ahead, behind = peers(1, g, b), peers(-1, g, b)
    ahead_too, behind_too = [
        [{"grp": (p["grp"] + 1) % 2, "blk": p["blk"]} for p in near[:DIRECT]] for near in (ahead, behind)
    ]
    tables = [
        pltpu.make_async_copy(src, dst, table_sem.at[n])
        for n, (src, dst) in enumerate(((lab_h, lab), (rate_h, rate)))
    ]
    loads = []
    for h in range(2):
        for f, src in enumerate((therm, moist)):
            loads.append(
                pltpu.make_async_copy(
                    src.at[:, pl.ds(h * HALF, HALF), :],
                    prof.at[h, :, :, pl.ds(f * LEV, LEV)],
                    load_sem.at[2 * h + f],
                )
            )
    for copy in tables + loads:
        copy.start()

    barrier = pltpu.get_barrier_semaphore()

    for o in reversed(range(1, PEERS)):
        pl.semaphore_signal(barrier, inc=1, device_id=ahead[o], device_id_type=MESH)
    for other in ahead_too + [left, right]:
        pl.semaphore_signal(barrier, inc=1, device_id=other, device_id_type=MESH)

    fields = []
    window = pl.multiple_of(g * (HALF - HALO), 8)
    for f, src in enumerate((zonal, merid, baro)):
        fields.append(
            pltpu.make_async_copy(
                src.at[:, pl.ds(window, WJ), :],
                stage.at[f, pl.ds(HALO, CX)],
                load_sem.at[4 + f],
            )
        )
    weights = [
        pltpu.make_async_copy(src.at[0], dst, weight_sem.at[n])
        for n, (src, dst) in enumerate(((w1h, w1), (w2h, w2), (w3h, w3), (w4h, w4)))
    ]
    for copy in fields + weights:
        copy.start()

    for copy in tables:
        copy.wait()
    slots[...] = slots_of(lab, ot, cum, rank, g, b)
    for copy in loads:
        copy.wait()

    for m in range(CHUNKS):
        want = lax.broadcasted_iota(jnp.int32, (CROWS, 128), 0) + m * CROWS
        hits = [jnp.where(slots[k : k + 1, :] == want, 1.0, 0.0).astype(BF) for k in range(16)]
        rows = jnp.dot(
            jnp.concatenate(hits, axis=1),
            prof[...].reshape(COLS, 2 * LEV),
            preferred_element_type=F32,
        )
        send[m * CROWS : (m + 1) * CROWS, :] = rows.astype(BF)
    recv[0:PIECE, :] = send[0:PIECE, :]
    pl.semaphore_wait(barrier, PEERS - 1 + DIRECT + 2)

    def piece(o):
        return pl.ds(o * PIECE, PIECE)

    def forth(o):
        return pltpu.make_async_remote_copy(
            src_ref=send.at[piece(o)],
            dst_ref=recv.at[piece(o)],
            send_sem=fs_sem,
            recv_sem=fr_sem.at[o // PER],
            device_id=ahead[o],
            device_id_type=MESH,
        )

    def home(o):
        return pltpu.make_async_remote_copy(
            src_ref=res.at[piece(o)],
            dst_ref=mine.at[piece(o)],
            send_sem=rs_sem,
            recv_sem=rr_sem.at[o // HPER],
            device_id=behind[o],
            device_id_type=MESH,
        )

    def direct(o):
        return pltpu.make_async_remote_copy(
            src_ref=res.at[piece(o)],
            dst_ref=theirs.at[piece(o)],
            send_sem=ds_sem,
            recv_sem=dr_sem,
            device_id=behind_too[o],
            device_id_type=MESH,
        )

    def bulk(ref, first, last, send_sem, recv_sem):
        rows = ref.at[pl.ds(first * PIECE, (last - first) * PIECE)]
        return pltpu.make_async_remote_copy(
            src_ref=rows,
            dst_ref=rows,
            send_sem=send_sem,
            recv_sem=recv_sem,
            device_id=partner,
            device_id_type=MESH,
        )

    def across(k):
        rows = pl.ds(k * HROWS, HROWS)
        return pltpu.make_async_remote_copy(
            src_ref=mine.at[rows],
            dst_ref=theirs.at[rows],
            send_sem=ps_sem,
            recv_sem=pr_sem.at[k // LAST],
            device_id=partner,
            device_id_type=MESH,
        )

    def each(first, last, act):
        for o in range(first, last):
            act(o)

    each(1, PEERS, lambda o: forth(o).start())
    halos = [
        pltpu.make_async_remote_copy(
            src_ref=stage.at[:, pl.ds(src, HALO)],
            dst_ref=stage.at[:, pl.ds(dst, HALO)],
            send_sem=hs_sem.at[n],
            recv_sem=hr_sem.at[n],
            device_id=other,
            device_id_type=MESH,
        )
        for n, (src, dst, other) in enumerate(((CX, 0, right), (HALO, HALO + CX, left)))
    ]
    places = slots[pl.ds(pl.multiple_of(g * 8, 8), 8), :].astype(F32)
    columns = jnp.transpose(places).astype(jnp.int32)
    lane = lax.broadcasted_iota(jnp.int32, (128, 2 * MINE), 1)
    for k in range(8):
        hit = jnp.where(columns[:, k : k + 1] == lane, 1.0, 0.0)
        goal[k * 128 : (k + 1) * 128, :] = hit.astype(BF)
    for copy in fields:
        copy.wait()

    def widen(i, carry):
        east[i] = stage[0, i].astype(F32)
        north[i] = stage[1, i].astype(F32)
        press[i] = stage[2, i].astype(F32)
        return carry

    half = jnp.broadcast_to(rate[...] * 0.5, (WJ, LEV))
    lax.fori_loop(HALO, HALO + CX, widen, 0)
    for s in range(2, 2 * SUB + 2, 2):
        advance(half, east, north, press, (s + 7, ROWS - 7 - s), (s + 8, ROWS - 8 - s))
    for copy in weights:
        copy.wait()

    def hand_on(k):
        bulk(mine, max(k * HPER, 1), (k + 1) * HPER, rs_sem, rr_sem.at[k]).wait_recv()
        across(k).start()

    def network(k):
        rows = pl.ds(k * CROWS, CROWS)
        x = recv[rows, :]
        for n in range(2):
            cut = slice(n * 512, (n + 1) * 512)
            hid_a[:, cut] = silu(jnp.dot(x, w1[:, cut], preferred_element_type=F32)).astype(BF)
        for n in range(2):
            cut = slice(n * 512, (n + 1) * 512)
            hid_b[:, cut] = silu(jnp.dot(hid_a[...], w2[:, cut], preferred_element_type=F32)).astype(BF)
        for n in range(2):
            cut = slice(n * 512, (n + 1) * 512)
            hid_a[:, cut] = silu(jnp.dot(hid_b[...], w3[:, cut], preferred_element_type=F32)).astype(BF)
        res[rows, :] = jnp.dot(hid_a[...], w4[...], preferred_element_type=F32).astype(BF)

    for k in range(CHUNKS):
        bulk(recv, max(k * PER, 1), (k + 1) * PER, fs_sem, fr_sem.at[k]).wait_recv()
        network(k)
        each(max(k * PER, 1), (k + 1) * PER, lambda o: home(o).start())
        each(k * PER, min((k + 1) * PER, DIRECT), lambda o: direct(o).start())
        if k == 0:
            mine[0:PIECE, :] = res[0:PIECE, :]

    own = pl.ds(pl.multiple_of(g * HALO, 8), HALF)

    def narrow(i, carry):
        east_o[i] = east[i + HALO, own].astype(BF)
        north_o[i] = north[i + HALO, own].astype(BF)
        press_o[i] = press[i + HALO, own].astype(BF)
        return carry

    for copy in halos:
        copy.start()
    for k in range(FIRST, HANDS):
        hand_on(k)
    for copy in halos:
        copy.wait()
    lax.fori_loop(0, HALO, widen, 0)
    lax.fori_loop(HALO + CX, ROWS, widen, 0)
    for s in range(2, 2 * SUB + 2, 2):
        advance(half, east, north, press, (s - 1, s + 7), (s, s + 8))
        advance(half, east, north, press, (ROWS - 7 - s, ROWS + 1 - s), (ROWS - 8 - s, ROWS - s))
    lax.fori_loop(0, CX, narrow, 0)
    for k in range(FIRST):
        bulk(mine, max(k * HPER, 1), (k + 1) * HPER, rs_sem, rr_sem.at[k]).wait_recv()
    bulk(theirs, 0, DIRECT, ds_sem, dr_sem).wait_recv()
    bulk(theirs, DIRECT, LAST * HPER, ps_sem, pr_sem.at[0]).wait_recv()
    early = MINE + LAST * HROWS
    for k in range(4):
        cut = slice(k * 256, (k + 1) * 256)
        acc[cut, :] = jnp.dot(goal[cut, :early], back[:early, :], preferred_element_type=F32)
    bulk(theirs, LAST * HPER, PEERS, ps_sem, pr_sem.at[1]).wait_recv()
    for k in range(4):
        cut = slice(k * 256, (k + 1) * 256)
        rows = acc[cut, :] + jnp.dot(goal[cut, early:], back[early:, :], preferred_element_type=F32)
        heat_o[cut, :] = rows[:, :LEV].astype(BF)
        moist_o[cut, :] = rows[:, LEV:].astype(BF)
    bulk(theirs, DIRECT, PEERS, ps_sem, pr_sem.at[0]).wait_send()
    bulk(theirs, 0, DIRECT, ds_sem, dr_sem).wait_send()
    bulk(send, 1, PEERS, fs_sem, fr_sem.at[0]).wait_send()
    bulk(res, 1, PEERS, rs_sem, rr_sem.at[0]).wait_send()


def store_kernel(*refs):
    sources, targets, sem = refs[:5], refs[5:10], refs[10]
    copies = [
        pltpu.make_async_copy(src, dst, sem.at[n])
        for n, (src, dst) in enumerate(zip(sources, targets))
    ]
    for copy in copies:
        copy.start()
    for copy in copies:
        copy.wait()


def local(zonal, merid, baro, therm, moist, labels, rate, w1, w2, w3, w4):
    vmem = pl.BlockSpec(memory_space=pltpu.VMEM)
    hbm = pl.BlockSpec(memory_space=pltpu.HBM)
    field = jax.ShapeDtypeStruct((CX, HALF, LEV), BF)
    dma = pltpu.SemaphoreType.DMA
    hid = w2.shape[-1]
    flat = jax.ShapeDtypeStruct((CX * HALF, LEV), BF)
    kinds = (field, field, field, flat, flat)
    inputs = [
        pltpu.with_memory_space_constraint(a, pltpu.HBM)
        for a in (labels, rate.reshape(1, LEV), therm, moist, zonal, merid, baro, w1, w2, w3, w4)
    ]
    results = pl.pallas_call(
        main_kernel,
        out_shape=kinds,
        in_specs=[hbm] * 11,
        out_specs=(vmem,) * 5,
        scratch_shapes=[
            pltpu.VMEM((CX, 2 * HALF), jnp.int32),
            pltpu.VMEM((1, LEV), F32),
            pltpu.VMEM((16, 128), jnp.int32),
            pltpu.VMEM((2 * MINE, 2 * LEV), BF),
            pltpu.VMEM((CX * HALF, 2 * MINE), BF),
            pltpu.VMEM((CX * HALF, 2 * LEV), F32),
            pltpu.VMEM((2, CX, HALF, 2 * LEV), BF),
            pltpu.VMEM((1024, 128), BF),
            pltpu.VMEM((1024, 256), F32),
            pltpu.VMEM((16, 128), F32),
            pltpu.VMEM((MINE, 2 * LEV), BF),
            pltpu.VMEM((MINE, 2 * LEV), BF),
            pltpu.VMEM((MINE, 2 * LEV), BF),
            pltpu.VMEM((CROWS, hid), BF),
            pltpu.VMEM((CROWS, hid), BF),
            pltpu.VMEM(w1.shape[1:], BF),
            pltpu.VMEM(w2.shape[1:], BF),
            pltpu.VMEM(w3.shape[1:], BF),
            pltpu.VMEM(w4.shape[1:], BF),
            pltpu.VMEM((3, ROWS, WJ, LEV), BF),
            pltpu.VMEM((ROWS, WJ, LEV), F32),
            pltpu.VMEM((ROWS, WJ, LEV), F32),
            pltpu.VMEM((ROWS, WJ, LEV), F32),
            dma((2,)), dma((7,)), dma((4,)), dma, dma,
            dma, dma((CHUNKS,)), dma, dma((HANDS,)),
            dma, dma((2,)), dma((2,)), dma((2,)),
        ],
        compiler_params=pltpu.CompilerParams(
            collective_id=0, has_side_effects=True, vmem_limit_bytes=40 * 1024 * 1024
        ),
        name="main",
    )(*inputs)
    east, north, press, heat, moistening = pl.pallas_call(
        store_kernel,
        out_shape=kinds,
        in_specs=[vmem] * 5,
        out_specs=(hbm,) * 5,
        scratch_shapes=[dma((5,))],
        compiler_params=pltpu.CompilerParams(vmem_limit_bytes=4 * 1024 * 1024),
        name="store",
    )(*results)
    return east, north, press, heat.reshape(CX, HALF, LEV), moistening.reshape(CX, HALF, LEV)


def solution(mesh):
    whole = P("blk", None, None)
    out = P("blk", "grp", None)
    return jax.shard_map(
        local,
        mesh=mesh,
        in_specs=(whole,) * 5 + (P("blk", None), P()) + (whole,) * 4,
        out_specs=(out,) * 5,
        check_vma=False,
    )
```
